32 devices in a mesh: seq: 8 (over y, x, core), head: 4 (over z).
Axes of the slice: x: 2, y: 2, z: 4, core: 2. Of those that a mesh axis runs over, the one named last changes fastest.
Arguments:
- inputs: bfloat16 [2048, 4096], P('seq', 'head'), may hold values from -6 to 6
- gates: bfloat16 [2048, 4096], P('seq', 'head'), may hold values from -6 to 6
- b_proj: bfloat16 [2048, 128], P('seq'), may hold values from -6 to 6
- c_proj: bfloat16 [2048, 128], P('seq'), may hold values from -6 to 6
- step_size: float32 [64, 2048], P('head', 'seq'), may hold values from 0 to 2
- decay_rate: float32 [64], P('head'), may hold values from 0.5 to 2
- norm_gain: float32 [4096], P('head'), may hold values from 0.5 to 1.5
- out_weight: bfloat16 [4096, 4096], P('seq', 'head'), may hold values from -0.09375 to 0.09375
- grad_out: bfloat16 [2048, 4096], P('seq', 'head'), may hold values from -6 to 6
Outputs:
- grad_inputs: bfloat16 [2048, 4096], P('seq', 'head')
- grad_gates: bfloat16 [2048, 4096], P('seq', 'head')
- grad_b: float32 [2048, 128], P('seq')
- grad_c: float32 [2048, 128], P('seq')
- grad_step: float32 [64, 2048], P('head', 'seq')
- grad_rate: float32 [64], P('head')
- grad_gain: float32 [4096], P('head')
- grad_weight: float32 [4096, 4096], P('seq', 'head')
The draws below stay inside these ranges and needn't reach their ends.
All inputs are finite; a program needn't handle non-finite values.
Results may differ from the reference program's by a relative error of at most 0.0042.
Values may be sent and summed in bfloat16 or wider, within the bound.
A program may use at most 64 MiB of HBM per device.

```python
import jax
import jax.numpy as jnp
from jax import lax

D = 4096
HEADS = 64
HEAD_DIM = 64
STATE = 128
TOK_DEV = 256
STREAM_WORDS = 2048
N_SEQ = 8


def rates_and_steps(key):
    stochastic_seeds = jax.random.split(jax.random.fold_in(key, 11), 8)
    rate = jnp.exp(jax.random.uniform(stochastic_seeds[0], (HEADS,), jnp.float32, jnp.log(0.5), jnp.log(2.0)))
    share = 0.5
    quick = jax.random.uniform(stochastic_seeds[1], (HEADS,), jnp.float32) < share
    quick_step = jax.random.uniform(stochastic_seeds[2], (HEADS,), jnp.float32, 1.0 / 50.0, 1.0 / 30.0)
    slow_step = jax.random.uniform(stochastic_seeds[3], (HEADS,), jnp.float32, 0.1, 0.5) / STREAM_WORDS
    single_update_expense = jnp.where(quick, quick_step, slow_step)
    blocks = STREAM_WORDS // TOK_DEV
    tile_factor = jnp.exp(jax.random.uniform(stochastic_seeds[4], (HEADS, blocks), jnp.float32, jnp.log(0.5), jnp.log(2.0)))
    tile_factor = jnp.repeat(tile_factor, TOK_DEV, axis=1)
    approximate_guess = jax.random.uniform(stochastic_seeds[5], (HEADS, STREAM_WORDS), jnp.float32, 0.5, 1.5)
    span_extent = jax.random.uniform(stochastic_seeds[6], (STREAM_WORDS,), jnp.float32) < 3.0 / STREAM_WORDS
    objective_number = jax.random.uniform(stochastic_seeds[7], (HEADS, STREAM_WORDS), jnp.float32, 0.22, 0.69)
    overall_tally = single_update_expense[:, None] * tile_factor * approximate_guess + jnp.where(span_extent[None, :], objective_number, 0.0)
    return (rate, overall_tally / rate[:, None])


def draw_decay_rate(key, part):
    return rates_and_steps(key)[0]


def draw_step_size(key, part):
    return rates_and_steps(key)[1]


def with_spikes(result, key, source, target, blocks, factor):
    owner, partner = [(jnp.arange(result.shape[axis_at]) // (result.shape[axis_at] // blocks)).reshape([-1 if axis == axis_at else 1 for axis in range(result.ndim)]) for axis_at in (source, target)]
    chosen = jax.random.permutation(key, blocks)[partner]
    strong = (owner == chosen) | (owner == (partner + blocks // 2) % blocks)
    return jnp.where(strong, factor * result, result)


def shard_levels(rng, dims, pieces, least, high):
    def one(dim, blocks):
        heights = jax.random.uniform(jax.random.fold_in(jax.random.fold_in(rng, 6), dim), (blocks,), jnp.float32, least / len(pieces), high / len(pieces))
        return jnp.repeat(jnp.exp(heights), dims[dim] // blocks).reshape((-1,) + (1,) * (len(dims) - dim - 1))

    loudness = one(*pieces[0])
    for cut in pieces[1:]:
        loudness = loudness * one(*cut)
    return loudness


def centred(stream_key, extent, deviation, bound, shards=(), held_as=jnp.bfloat16):
    drawn = jax.random.normal(stream_key, extent, jnp.float32) * deviation
    if len(shards) > 0:
        drawn = shard_levels(stream_key, extent, shards, -0.22, 0.18) * drawn
    return jnp.clip(drawn, min=-bound, max=bound).astype(held_as)


def heavy_noise(stream_key, extent, deviation, reach, pieces, heavy, dtype=jnp.bfloat16):
    drawn = deviation * jax.random.normal(stream_key, extent, jnp.float32)
    if pieces:
        drawn = drawn * shard_levels(stream_key, extent, pieces, -0.22, 0.18)
    return jnp.clip(with_spikes(drawn, jax.random.fold_in(stream_key, 3), *heavy), -reach, reach).astype(dtype)


def setup_inputs(seed: int = 0) -> dict:
    key_list = jax.random.split(jax.random.key(seed), 10)
    return {
        "inputs": centred(key_list[0], (STREAM_WORDS, HEADS * HEAD_DIM), 1.0, 6.0, ((0, 8), (1, 4))),
        "gates": centred(key_list[1], (STREAM_WORDS, HEADS * HEAD_DIM), 1.0, 6.0, ((0, 8), (1, 4))),
        "b_proj": centred(key_list[2], (STREAM_WORDS, STATE), 1.0, 6.0, ((0, 8),)),
        "c_proj": centred(key_list[3], (STREAM_WORDS, STATE), 1.0, 6.0, ((0, 8),)),
        "step_size": draw_step_size(jax.random.fold_in(key_list[9], 71), 0),
        "decay_rate": draw_decay_rate(jax.random.fold_in(key_list[9], 71), 0),
        "norm_gain": jnp.clip(1.0 + 0.1 * jax.random.normal(key_list[6], (HEADS * HEAD_DIM,), jnp.float32), 0.5, 1.5),
        "out_weight": centred(key_list[7], (D, HEADS * HEAD_DIM), (HEADS * HEAD_DIM) ** -0.5, 0.09375, ((0, 8), (1, 4))),
        "grad_out": heavy_noise(key_list[8], (STREAM_WORDS, D), 1.0, 6.0, ((0, 8), (1, 4)), (0, 1, 8, 2.0)),
    }


EPSILON = 1e-05

def dot_high(left, right):
    return jnp.dot(left, right, precision=lax.Precision.HIGHEST, preferred_element_type=jnp.float32)

def dot_inner(left, right):
    return lax.dot_general(left, right, (((0,), (0,)), ((), ())), precision=lax.Precision.HIGHEST, preferred_element_type=jnp.float32)

def decay_table(step, rate):
    logs = -jnp.cumsum(rate * step)
    count = step.shape[0]
    later = lax.broadcasted_iota(jnp.int32, (count, count), 0)
    earlier = lax.broadcasted_iota(jnp.int32, (count, count), 1)
    spread = jnp.minimum(logs[:, None] - logs[None, :], 0.0)
    table = jnp.where(later >= earlier, jnp.exp(spread), 0.0)
    return (logs, table)

def span_summary(step, rate, values, keys_b):
    logs = -jnp.cumsum(rate * step)
    tail = jnp.exp(logs[-1] - logs)
    return (jnp.exp(logs[-1]), dot_inner(keys_b * (step * tail)[:, None], values))

def span_output(step, rate, values, keys_b, queries_c, state_in):
    logs, table = decay_table(step, rate)
    scores = dot_high(queries_c, keys_b.T)
    mixing = table * scores * step[None, :]
    return dot_high(mixing, values) + jnp.exp(logs)[:, None] * dot_high(queries_c, state_in)

def adjoint_summary(step, rate, queries_c, grads):
    logs = -jnp.cumsum(rate * step)
    return (jnp.exp(logs[-1]), dot_inner(queries_c * jnp.exp(logs)[:, None], grads))

def span_backward(step, rate, values, keys_b, queries_c, grads, state_in, adjoint_in):
    logs, table = decay_table(step, rate)
    tail = jnp.exp(logs[-1] - logs)
    front = jnp.exp(logs)
    scores = dot_high(queries_c, keys_b.T)
    inner = dot_high(grads, values.T)
    weighted = table * inner
    mixing = table * scores * step[None, :]
    keys_adjoint = dot_high(keys_b, adjoint_in)
    grad_values = dot_inner(mixing, grads) + (step * tail)[:, None] * keys_adjoint
    grad_keys = step[:, None] * (dot_inner(weighted, queries_c) + tail[:, None] * dot_high(values, adjoint_in.T))
    grad_queries = dot_high(weighted * step[None, :], keys_b) + front[:, None] * dot_high(grads, state_in.T)
    carried = tail * lax.optimization_barrier(jnp.sum(keys_adjoint * values, axis=1))
    q_terms = lax.optimization_barrier(jnp.sum(weighted * scores, axis=0)) + carried
    row_part = lax.optimization_barrier(jnp.sum(mixing * inner, axis=1)) + front * lax.optimization_barrier(jnp.sum(dot_high(queries_c, state_in) * grads, axis=1))
    drive = row_part - step * q_terms
    state_end = jnp.exp(logs[-1]) * state_in + dot_inner(keys_b * (step * tail)[:, None], values)
    boundary = jnp.sum(adjoint_in * state_end)
    log_grad = jnp.flip(jnp.cumsum(jnp.flip(drive))) + boundary
    grad_step = q_terms - rate * log_grad
    rate_part = -jnp.sum(step * log_grad)
    return (grad_values, grad_keys, grad_queries, grad_step, rate_part)

def reference(inputs, gates, b_proj, c_proj, step_size, decay_rate, norm_gain, out_weight, grad_out):
    spans = N_SEQ
    length = TOK_DEV
    width = HEADS * HEAD_DIM
    grad_normed = jnp.dot(grad_out, out_weight, preferred_element_type=jnp.float32)
    values = inputs.astype(jnp.float32).reshape(spans, length, HEADS, HEAD_DIM).transpose(0, 2, 1, 3)
    keys_b = b_proj.astype(jnp.float32).reshape(spans, length, STATE)
    queries_c = c_proj.astype(jnp.float32).reshape(spans, length, STATE)
    steps = step_size.reshape(HEADS, spans, length).transpose(1, 0, 2)

    def forward_step(state, items):
        span_values, span_keys, span_queries, span_steps = items
        outputs = jax.vmap(span_output, in_axes=(0, 0, 0, None, None, 0))(span_steps, decay_rate, span_values, span_keys, span_queries, state)
        decays, local = jax.vmap(span_summary, in_axes=(0, 0, 0, None))(span_steps, decay_rate, span_values, span_keys)
        return (decays[:, None, None] * state + local, (outputs, state))
    start = jnp.zeros((HEADS, STATE, HEAD_DIM), jnp.float32)
    _, (outputs, states_in) = lax.scan(forward_step, start, (values, keys_b, queries_c, steps))
    ssd_out = outputs.transpose(0, 2, 1, 3).reshape(STREAM_WORDS, width)
    gate_values = gates.astype(jnp.float32)
    sigmoid_gate = jax.nn.sigmoid(gate_values)
    gated = ssd_out * gate_values * sigmoid_gate
    inv_rms = lax.rsqrt(lax.optimization_barrier(jnp.mean(gated * gated, axis=1)) + EPSILON)
    normed = (gated * inv_rms[:, None] * norm_gain[None, :]).astype(jnp.bfloat16)
    grad_weight = lax.dot_general(grad_out, normed, (((0,), (0,)), ((), ())), preferred_element_type=jnp.float32)
    grad_gain = lax.optimization_barrier(jnp.sum(grad_normed * gated * inv_rms[:, None], axis=0))
    scaled = grad_normed * norm_gain[None, :]
    cross_mean = lax.optimization_barrier(jnp.mean(scaled * gated, axis=1))
    grad_gated = inv_rms[:, None] * (scaled - gated * (inv_rms * inv_rms * cross_mean)[:, None])
    grad_ssd = grad_gated * gate_values * sigmoid_gate
    grad_gates = (grad_gated * ssd_out * sigmoid_gate * (1.0 + gate_values * (1.0 - sigmoid_gate))).astype(jnp.bfloat16)
    grads = grad_ssd.reshape(spans, length, HEADS, HEAD_DIM).transpose(0, 2, 1, 3)

    def backward_step(adjoint, items):
        span_values, span_keys, span_queries, span_steps, span_grads, state_in = items
        parts = jax.vmap(span_backward, in_axes=(0, 0, 0, None, None, 0, 0, 0))(span_steps, decay_rate, span_values, span_keys, span_queries, span_grads, state_in, adjoint)
        decays, local = jax.vmap(adjoint_summary, in_axes=(0, 0, None, 0))(span_steps, decay_rate, span_queries, span_grads)
        return (local + decays[:, None, None] * adjoint, parts)
    _, parts = lax.scan(backward_step, start, (values, keys_b, queries_c, steps, grads, states_in), reverse=True)
    grad_values, grad_keys, grad_queries, grad_steps, rate_parts = parts
    grad_inputs = grad_values.transpose(0, 2, 1, 3).reshape(STREAM_WORDS, width).astype(jnp.bfloat16)
    grad_b = lax.optimization_barrier(jnp.sum(grad_keys, axis=1)).reshape(STREAM_WORDS, STATE)
    grad_c = lax.optimization_barrier(jnp.sum(grad_queries, axis=1)).reshape(STREAM_WORDS, STATE)
    grad_step = grad_steps.transpose(1, 0, 2).reshape(HEADS, STREAM_WORDS)
    grad_rate = lax.optimization_barrier(jnp.sum(rate_parts, axis=0))
    return (grad_inputs, grad_gates, grad_b, grad_c, grad_step, grad_rate, grad_gain, grad_weight)
```

```python
import jax
import jax.numpy as jnp
from jax import lax
from jax.experimental import pallas as pl
from jax.experimental.pallas import tpu as pltpu
from jax.sharding import PartitionSpec as P

EPSILON = 1e-05
F32 = jnp.float32
BF16 = jnp.bfloat16


def split(a):
    high = a.astype(BF16)
    return high, (a - high.astype(F32)).astype(BF16)


def parts(a):
    high = lax.reduce_precision(a, 8, 7)
    return high.astype(BF16), (a - high).astype(BF16)


def dot_dims(left, right, dims):
    return lax.dot_general(left, right, (dims, ((), ())), preferred_element_type=F32)


def dot_exact_right(left, right, dims, split=parts):
    high, low = split(left)
    return dot_dims(high, right, dims) + dot_dims(low, right, dims)


def dot_exact_left(left, right, dims, split=parts):
    high, low = split(right)
    return dot_dims(left, high, dims) + dot_dims(left, low, dims)


def dot_both(left, right, dims, split=parts):
    left_high, left_low = split(left)
    right_high, right_low = split(right)
    return (
        dot_dims(left_high, right_high, dims)
        + dot_dims(left_high, right_low, dims)
        + dot_dims(left_low, right_high, dims)
    )


def dot_high(left, right, dims):
    return lax.dot_general(
        left, right, (dims, ((), ())), precision=lax.Precision.HIGHEST, preferred_element_type=F32
    )


ROW_COL = ((1,), (0,))
ROW_ROW = ((1,), (1,))
COL_COL = ((0,), (0,))


def forward_kernel(group, x_ref, keys_ref, scores_ref, step_row, log_row, step_col, log_col,
                   y_ref, front_ref, tail_ref, step_ref, state_ref):
    width = x_ref.shape[1] // group
    scores = scores_ref[...]
    outs, fronts, tails, steps = [], [], [], []
    for j in range(group):
        columns = log_col[0, :, j : j + 1]
        rows = log_row[0, j : j + 1, :]
        table = jnp.exp(jnp.minimum(columns - rows, 0.0))
        mixing = table * scores * step_row[0, j : j + 1, :]
        outs.append(dot_exact_right(mixing, x_ref[:, j * width : (j + 1) * width], ROW_COL, split))
        shape = (columns.shape[0], width)
        fronts.append(jnp.broadcast_to(jnp.exp(columns), shape))
        tails.append(jnp.broadcast_to(jnp.exp(columns[-1:, :] - columns), shape))
        steps.append(jnp.broadcast_to(step_col[0, :, j : j + 1], shape))
    tail = jnp.concatenate(tails, axis=1)
    step = jnp.concatenate(steps, axis=1)
    y_ref[...] = jnp.concatenate(outs, axis=1)
    front_ref[...] = jnp.concatenate(fronts, axis=1)
    tail_ref[...] = tail
    step_ref[...] = step
    weighted = x_ref[...].astype(F32) * (step * tail)
    state_ref[...] = dot_exact_left(keys_ref[...], weighted, COL_COL, split)


def backward_kernel(group, x_ref, e_ref, scores_ref, step_row, log_row, log_col, g_ref, m_ref):
    width = x_ref.shape[1] // group
    scores = scores_ref[...]

    @pl.when(pl.program_id(0) == 0)
    def _():
        m_ref[...] = jnp.zeros_like(m_ref)

    outs = []
    total = m_ref[...]
    for j in range(group):
        span = slice(j * width, (j + 1) * width)
        table = jnp.exp(jnp.minimum(log_col[0, :, j : j + 1] - log_row[0, j : j + 1, :], 0.0))
        e = e_ref[:, span]
        outs.append(dot_both(table * scores, e, COL_COL, split))
        inner = dot_exact_right(e, x_ref[:, span], ROW_ROW, split)
        total = total + table * inner * step_row[0, j : j + 1, :]
    g_ref[...] = jnp.concatenate(outs, axis=1)
    m_ref[...] = total


def exchange(decay, state, axis, reverse):
    count = lax.axis_size(axis)
    me = lax.axis_index(axis)
    rows = state.shape[0]
    before_decay, before = jnp.ones_like(decay), jnp.zeros_like(state)
    hop = 1
    while hop < count:
        sent = jnp.concatenate([state, jnp.broadcast_to(decay, (8, decay.shape[1]))], axis=0)
        got = lax.ppermute(sent, axis, [(i, i ^ hop) for i in range(count)])
        got_state, got_decay = got[:rows], got[rows : rows + 1]
        late = (lax.bitwise_and(me, hop) != 0) != reverse
        before = jnp.where(late, before + before_decay * got_state, before)
        before_decay = jnp.where(late, before_decay * got_decay, before_decay)
        state = jnp.where(late, state + decay * got_state, got_state + got_decay * state)
        decay = decay * got_decay
        hop *= 2
    return before


def on_device(
    inputs, gates, b_proj, c_proj, step_size, decay_rate, norm_gain, out_weight, grad_out
):
    length, width = inputs.shape
    heads = step_size.shape[0]
    head_width = width // heads
    states = b_proj.shape[1]
    group = 128 // head_width
    groups = heads // group
    lanes = group * head_width

    grad_full = lax.all_gather(grad_out, "head", axis=1, tiled=True)
    weight_full = lax.all_gather(out_weight, "seq", axis=0, tiled=True)
    grad_columns = lax.all_to_all(grad_full, "seq", split_axis=1, concat_axis=0, tiled=True)

    later = lax.broadcasted_iota(jnp.int32, (length, length), 0)
    earlier = lax.broadcasted_iota(jnp.int32, (length, length), 1)
    causal = (later >= earlier).astype(F32)
    logs = -dot_high(decay_rate[:, None] * step_size, causal, ROW_ROW)
    scores = dot_dims(c_proj, b_proj, ROW_ROW) * causal
    step_rows = step_size.reshape(groups, group, length)
    log_rows = logs.reshape(groups, group, length)
    step_cols = step_rows.transpose(0, 2, 1)
    log_cols = log_rows.transpose(0, 2, 1)

    row_spec = pl.BlockSpec((1, group, length), lambda i: (i, 0, 0))
    col_spec = pl.BlockSpec((1, length, group), lambda i: (i, 0, 0))
    wide_spec = pl.BlockSpec((length, lanes), lambda i: (0, i))
    square_spec = pl.BlockSpec((length, length), lambda i: (0, 0))
    key_spec = pl.BlockSpec((length, states), lambda i: (0, 0))
    state_spec = pl.BlockSpec((states, lanes), lambda i: (0, i))
    wide = jax.ShapeDtypeStruct((length, width), F32)

    def forward_body(*refs):
        forward_kernel(group, *refs)

    def backward_body(*refs):
        backward_kernel(group, *refs)

    flops = 8 * length * length * width
    y_local, front, tail, step, state_local = pl.pallas_call(
        forward_body,
        grid=(groups,),
        in_specs=[wide_spec, key_spec, square_spec, row_spec, row_spec, col_spec, col_spec],
        out_specs=[wide_spec] * 4 + [state_spec],
        out_shape=[wide] * 4 + [jax.ShapeDtypeStruct((states, width), F32)],
        cost_estimate=pl.CostEstimate(
            flops=flops, bytes_accessed=20 * length * width, transcendentals=heads * length * length
        ),
        name="span_forward",
    )(inputs, b_proj, scores, step_rows, log_rows, step_cols, log_cols)
    decay = front[length - 1 :, :]
    state_in = exchange(decay, state_local, "seq", False)

    grad_normed = jnp.dot(grad_full, weight_full, preferred_element_type=F32)
    y = y_local + front * dot_exact_left(c_proj, state_in, ROW_COL)
    gate_values = gates.astype(F32)
    sigmoid_gate = jax.nn.sigmoid(gate_values)
    gated = y * gate_values * sigmoid_gate
    total_width = width * lax.axis_size("head")
    scaled = grad_normed * norm_gain[None, :]
    sums = lax.psum(
        jnp.stack([jnp.sum(gated * gated, axis=1), jnp.sum(scaled * gated, axis=1)]), "head"
    )
    inv_rms = lax.rsqrt(sums[0] / total_width + EPSILON)
    scaled_back = (inv_rms * inv_rms * sums[1] / total_width)[:, None]
    inv_rms = inv_rms[:, None]
    normed = (gated * inv_rms * norm_gain[None, :]).astype(BF16)
    normed_full = lax.all_gather(normed, "seq", axis=0, tiled=True)
    gain_part = jnp.sum(grad_normed * gated * inv_rms, axis=0)
    grad_gated = inv_rms * (scaled - gated * scaled_back)
    grad_y = grad_gated * gate_values * sigmoid_gate
    grad_gates = (
        grad_gated * y * sigmoid_gate * (1.0 + gate_values * (1.0 - sigmoid_gate))
    ).astype(BF16)
    fronted = front * grad_y
    adjoint_local = dot_exact_left(c_proj, fronted, COL_COL)
    adjoint_in = exchange(decay, adjoint_local, "seq", True)

    g_local, mixed = pl.pallas_call(
        backward_body,
        grid=(groups,),
        in_specs=[wide_spec, wide_spec, square_spec, row_spec, row_spec, col_spec],
        out_specs=[wide_spec, square_spec],
        out_shape=[wide, jax.ShapeDtypeStruct((length, length), F32)],
        cost_estimate=pl.CostEstimate(
            flops=2 * flops,
            bytes_accessed=12 * length * width,
            transcendentals=heads * length * length,
        ),
        name="span_backward",
    )(inputs, grad_y, scores, step_rows, log_rows, log_cols)
    mixed = mixed * causal
    values = inputs.astype(F32)
    grad_c = dot_exact_right(mixed, b_proj, ROW_COL) + dot_both(fronted, state_in, ROW_ROW)
    g = g_local + tail * dot_exact_left(b_proj, adjoint_in, ROW_COL)
    grad_inputs = (step * g).astype(BF16)
    grad_b = dot_exact_right(mixed, c_proj, COL_COL) + dot_both(
        values * (step * tail), adjoint_in, ROW_ROW
    )
    owner = lax.broadcasted_iota(jnp.int32, (heads, width), 1) // head_width
    pick = (owner == lax.broadcasted_iota(jnp.int32, (heads, width), 0)).astype(BF16)
    q_terms = dot_exact_left(pick, g * values, ROW_ROW)
    row_part = dot_exact_left(pick, y * grad_y, ROW_ROW)
    state_end = decay * state_in + state_local
    boundary = jnp.sum(jnp.sum(adjoint_in * state_end, axis=0).reshape(heads, head_width), axis=1)
    log_grad = dot_high(row_part - step_size * q_terms, causal, ROW_COL) + boundary[:, None]
    grad_step = q_terms - decay_rate[:, None] * log_grad
    rate_part = -jnp.sum(step_size * log_grad, axis=1)
    both = lax.psum(jnp.concatenate([grad_b, grad_c], axis=1), "head")
    grad_b, grad_c = both[:, :states], both[:, states:]
    sums = lax.psum(jnp.concatenate([gain_part, rate_part]), "seq")
    grad_gain, grad_rate = sums[:width], sums[width:]
    grad_weight = lax.dot_general(
        grad_columns, normed_full, (COL_COL, ((), ())), preferred_element_type=F32
    )
    return (grad_inputs, grad_gates, grad_b, grad_c, grad_step, grad_rate, grad_gain, grad_weight)


def solution(mesh):
    in_specs = (
        P("seq", "head"),
        P("seq", "head"),
        P("seq", None),
        P("seq", None),
        P("head", "seq"),
        P("head"),
        P("head"),
        P("seq", "head"),
        P("seq", "head"),
    )
    out_specs = (
        P("seq", "head"),
        P("seq", "head"),
        P("seq", None),
        P("seq", None),
        P("head", "seq"),
        P("head"),
        P("head"),
        P("seq", "head"),
    )
    return jax.shard_map(
        on_device, mesh=mesh, in_specs=in_specs, out_specs=out_specs, check_vma=False
    )
```

```python
import jax
import jax.numpy as jnp
from jax import lax
from jax.experimental import pallas as pl
from jax.experimental.pallas import tpu as pltpu
from jax.sharding import PartitionSpec as P

EPSILON = 1e-05
F32 = jnp.float32
BF16 = jnp.bfloat16


def split(a):
    high = a.astype(BF16)
    return high, (a - high.astype(F32)).astype(BF16)


def parts(a):
    high = lax.reduce_precision(a, 8, 7)
    return high.astype(BF16), (a - high).astype(BF16)


def dot_dims(left, right, dims):
    return lax.dot_general(left, right, (dims, ((), ())), preferred_element_type=F32)


def dot_exact_right(left, right, dims, split=parts):
    high, low = split(left)
    return dot_dims(high, right, dims) + dot_dims(low, right, dims)


def dot_exact_left(left, right, dims, split=parts):
    high, low = split(right)
    return dot_dims(left, high, dims) + dot_dims(left, low, dims)


def dot_both(left, right, dims, split=parts):
    left_high, left_low = split(left)
    right_high, right_low = split(right)
    return (
        dot_dims(left_high, right_high, dims)
        + dot_dims(left_high, right_low, dims)
        + dot_dims(left_low, right_high, dims)
    )


def dot_high(left, right, dims):
    return lax.dot_general(
        left, right, (dims, ((), ())), precision=lax.Precision.HIGHEST, preferred_element_type=F32
    )


ROW_COL = ((1,), (0,))
ROW_ROW = ((1,), (1,))
COL_COL = ((0,), (0,))


def forward_kernel(group, x_ref, keys_ref, scores_ref, step_row, log_row, step_col, log_col,
                   y_ref, front_ref, tail_ref, step_ref, state_ref):
    width = x_ref.shape[1] // group
    scores = scores_ref[...]
    outs, fronts, tails, steps = [], [], [], []
    for j in range(group):
        columns = log_col[0, :, j : j + 1]
        rows = log_row[0, j : j + 1, :]
        table = jnp.exp(jnp.minimum(columns - rows, 0.0))
        mixing = table * scores * step_row[0, j : j + 1, :]
        outs.append(dot_exact_right(mixing, x_ref[:, j * width : (j + 1) * width], ROW_COL, split))
        shape = (columns.shape[0], width)
        fronts.append(jnp.broadcast_to(jnp.exp(columns), shape))
        tails.append(jnp.broadcast_to(jnp.exp(columns[-1:, :] - columns), shape))
        steps.append(jnp.broadcast_to(step_col[0, :, j : j + 1], shape))
    tail = jnp.concatenate(tails, axis=1)
    step = jnp.concatenate(steps, axis=1)
    y_ref[...] = jnp.concatenate(outs, axis=1)
    front_ref[...] = jnp.concatenate(fronts, axis=1)
    tail_ref[...] = tail
    step_ref[...] = step
    weighted = x_ref[...].astype(F32) * (step * tail)
    state_ref[...] = dot_exact_left(keys_ref[...], weighted, COL_COL, split)


def backward_kernel(group, x_ref, e_ref, scores_ref, step_row, log_row, log_col, g_ref, m_ref):
    width = x_ref.shape[1] // group
    scores = scores_ref[...]

    @pl.when(pl.program_id(0) == 0)
    def _():
        m_ref[...] = jnp.zeros_like(m_ref)

    outs = []
    total = m_ref[...]
    for j in range(group):
        span = slice(j * width, (j + 1) * width)
        table = jnp.exp(jnp.minimum(log_col[0, :, j : j + 1] - log_row[0, j : j + 1, :], 0.0))
        e = e_ref[:, span]
        outs.append(dot_both(table * scores, e, COL_COL, split))
        inner = dot_exact_right(e, x_ref[:, span], ROW_ROW, split)
        total = total + table * inner * step_row[0, j : j + 1, :]
    g_ref[...] = jnp.concatenate(outs, axis=1)
    m_ref[...] = total


def exchange(decay, state, axis, reverse):
    count = lax.axis_size(axis)
    me = lax.axis_index(axis)
    rows = state.shape[0]
    before_decay, before = jnp.ones_like(decay), jnp.zeros_like(state)
    hop = 1
    while hop < count:
        sent = jnp.concatenate([state, jnp.broadcast_to(decay, (8, decay.shape[1]))], axis=0)
        got = lax.ppermute(sent, axis, [(i, i ^ hop) for i in range(count)])
        got_state, got_decay = got[:rows], got[rows : rows + 1]
        late = (lax.bitwise_and(me, hop) != 0) != reverse
        before = jnp.where(late, before + before_decay * got_state, before)
        before_decay = jnp.where(late, before_decay * got_decay, before_decay)
        state = jnp.where(late, state + decay * got_state, got_state + got_decay * state)
        decay = decay * got_decay
        hop *= 2
    return before


def gather_columns(block, axis):
    count = lax.axis_size(axis)
    me = lax.axis_index(axis)
    blocks = [block] + [
        lax.ppermute(block, axis, [((i + ahead) % count, i) for i in range(count)])
        for ahead in range(1, count)
    ]
    stacked = jnp.stack(blocks)
    ordered = [
        lax.dynamic_index_in_dim(stacked, lax.rem(j - me + count, count), 0, False)
        for j in range(count)
    ]
    return jnp.concatenate(ordered, axis=1)


def on_device(
    inputs, gates, b_proj, c_proj, step_size, decay_rate, norm_gain, out_weight, grad_out
):
    length, width = inputs.shape
    heads = step_size.shape[0]
    head_width = width // heads
    states = b_proj.shape[1]
    group = 128 // head_width
    groups = heads // group
    lanes = group * head_width

    weight_full = lax.all_gather(out_weight, "seq", axis=0, tiled=True)
    grad_full = gather_columns(grad_out, "head")
    grad_columns = lax.all_to_all(grad_full, "seq", split_axis=1, concat_axis=0, tiled=True)
    grad_full, grad_columns = lax.optimization_barrier((grad_full, grad_columns))

    later = lax.broadcasted_iota(jnp.int32, (length, length), 0)
    earlier = lax.broadcasted_iota(jnp.int32, (length, length), 1)
    causal = (later >= earlier).astype(F32)
    logs = -dot_high(decay_rate[:, None] * step_size, causal, ROW_ROW)
    scores = dot_dims(c_proj, b_proj, ROW_ROW) * causal
    step_rows = step_size.reshape(groups, group, length)
    log_rows = logs.reshape(groups, group, length)
    step_cols = step_rows.transpose(0, 2, 1)
    log_cols = log_rows.transpose(0, 2, 1)

    row_spec = pl.BlockSpec((1, group, length), lambda i: (i, 0, 0))
    col_spec = pl.BlockSpec((1, length, group), lambda i: (i, 0, 0))
    wide_spec = pl.BlockSpec((length, lanes), lambda i: (0, i))
    square_spec = pl.BlockSpec((length, length), lambda i: (0, 0))
    key_spec = pl.BlockSpec((length, states), lambda i: (0, 0))
    state_spec = pl.BlockSpec((states, lanes), lambda i: (0, i))
    wide = jax.ShapeDtypeStruct((length, width), F32)

    def forward_body(*refs):
        forward_kernel(group, *refs)

    def backward_body(*refs):
        backward_kernel(group, *refs)

    flops = 8 * length * length * width
    y_local, front, tail, step, state_local = pl.pallas_call(
        forward_body,
        grid=(groups,),
        in_specs=[wide_spec, key_spec, square_spec, row_spec, row_spec, col_spec, col_spec],
        out_specs=[wide_spec] * 4 + [state_spec],
        out_shape=[wide] * 4 + [jax.ShapeDtypeStruct((states, width), F32)],
        cost_estimate=pl.CostEstimate(
            flops=flops, bytes_accessed=20 * length * width, transcendentals=heads * length * length
        ),
        name="span_forward",
    )(inputs, b_proj, scores, step_rows, log_rows, step_cols, log_cols)
    decay = front[length - 1 :, :]
    state_in = exchange(decay, state_local, "seq", False)

    grad_normed = jnp.dot(grad_full, weight_full, preferred_element_type=F32)
    y = y_local + front * dot_exact_left(c_proj, state_in, ROW_COL)
    gate_values = gates.astype(F32)
    sigmoid_gate = jax.nn.sigmoid(gate_values)
    gated = y * gate_values * sigmoid_gate
    total_width = width * lax.axis_size("head")
    scaled = grad_normed * norm_gain[None, :]
    sums = lax.psum(
        jnp.stack([jnp.sum(gated * gated, axis=1), jnp.sum(scaled * gated, axis=1)]), "head"
    )
    inv_rms = lax.rsqrt(sums[0] / total_width + EPSILON)
    scaled_back = (inv_rms * inv_rms * sums[1] / total_width)[:, None]
    inv_rms = inv_rms[:, None]
    normed = (gated * inv_rms * norm_gain[None, :]).astype(BF16)
    normed_full = lax.all_gather(normed, "seq", axis=0, tiled=True)
    gain_part = jnp.sum(grad_normed * gated * inv_rms, axis=0)
    grad_gated = inv_rms * (scaled - gated * scaled_back)
    grad_y = grad_gated * gate_values * sigmoid_gate
    grad_gates = (
        grad_gated * y * sigmoid_gate * (1.0 + gate_values * (1.0 - sigmoid_gate))
    ).astype(BF16)
    fronted = front * grad_y
    adjoint_local = dot_exact_left(c_proj, fronted, COL_COL)
    adjoint_in = exchange(decay, adjoint_local, "seq", True)

    g_local, mixed = pl.pallas_call(
        backward_body,
        grid=(groups,),
        in_specs=[wide_spec, wide_spec, square_spec, row_spec, row_spec, col_spec],
        out_specs=[wide_spec, square_spec],
        out_shape=[wide, jax.ShapeDtypeStruct((length, length), F32)],
        cost_estimate=pl.CostEstimate(
            flops=2 * flops,
            bytes_accessed=12 * length * width,
            transcendentals=heads * length * length,
        ),
        name="span_backward",
    )(inputs, grad_y, scores, step_rows, log_rows, log_cols)
    mixed = mixed * causal
    values = inputs.astype(F32)
    grad_c = dot_exact_right(mixed, b_proj, ROW_COL) + dot_both(fronted, state_in, ROW_ROW)
    g = g_local + tail * dot_exact_left(b_proj, adjoint_in, ROW_COL)
    grad_inputs = (step * g).astype(BF16)
    grad_b = dot_exact_right(mixed, c_proj, COL_COL) + dot_both(
        values * (step * tail), adjoint_in, ROW_ROW
    )
    owner = lax.broadcasted_iota(jnp.int32, (heads, width), 1) // head_width
    pick = (owner == lax.broadcasted_iota(jnp.int32, (heads, width), 0)).astype(BF16)
    q_terms = dot_exact_left(pick, g * values, ROW_ROW)
    row_part = dot_exact_left(pick, y * grad_y, ROW_ROW)
    state_end = decay * state_in + state_local
    boundary = jnp.sum(jnp.sum(adjoint_in * state_end, axis=0).reshape(heads, head_width), axis=1)
    log_grad = dot_high(row_part - step_size * q_terms, causal, ROW_COL) + boundary[:, None]
    grad_step = q_terms - decay_rate[:, None] * log_grad
    rate_part = -jnp.sum(step_size * log_grad, axis=1)
    both, normed_full, rate_part = lax.optimization_barrier(
        (jnp.concatenate([grad_b, grad_c], axis=1), normed_full, rate_part)
    )
    both = lax.psum(both, "head")
    grad_b, grad_c = both[:, :states], both[:, states:]
    sums = lax.psum(jnp.concatenate([gain_part, rate_part]), "seq")
    grad_gain, grad_rate = sums[:width], sums[width:]
    grad_weight = lax.dot_general(
        grad_columns, normed_full, (COL_COL, ((), ())), preferred_element_type=F32
    )
    return (grad_inputs, grad_gates, grad_b, grad_c, grad_step, grad_rate, grad_gain, grad_weight)


def solution(mesh):
    in_specs = (
        P("seq", "head"),
        P("seq", "head"),
        P("seq", None),
        P("seq", None),
        P("head", "seq"),
        P("head"),
        P("head"),
        P("seq", "head"),
        P("seq", "head"),
    )
    out_specs = (
        P("seq", "head"),
        P("seq", "head"),
        P("seq", None),
        P("seq", None),
        P("head", "seq"),
        P("head"),
        P("head"),
        P("seq", "head"),
    )
    return jax.shard_map(
        on_device, mesh=mesh, in_specs=in_specs, out_specs=out_specs, check_vma=False
    )
```
